256 devices in a mesh: section: 8 (over y, x_hi), ep: 32 (over z, x_lo, core).
Axes of the slice: x: 4 (x_hi: 2, x_lo: 2; x = x_hi * 2 + x_lo), y: 4, z: 8, core: 2. Of those that a mesh axis runs over, the one named last changes fastest.
Arguments:
- handed: bfloat16 [8, 2, 2048, 7168], P('section', None, 'ep'), may hold values from -6 to 6
- routes: int32 [8, 2, 2048, 2], P('section', None, 'ep'), may hold values from 0 to 3, all different within a row; in each aligned block of 64 rows (0 to 63, 64 to 127, ..., all dimensions but the last counted through in order) at most 36 rows name the same one
- slot_order: int32 [8, 2, 32, 64], P('section', None, 'ep'), may hold values from 0 to 63, each once within a row
- gate_probs: float32 [8, 2, 2048, 2], P('section', None, 'ep'), may hold values from 0.2 to 1
- saved_gate: bfloat16 [8, 2, 32, 32, 36, 128], P('section', None, 'ep'), may hold values from -6 to 6
- saved_up: bfloat16 [8, 2, 32, 32, 36, 128], P('section', None, 'ep'), may hold values from -6 to 6
- w_gate: bfloat16 [8, 32, 896, 1024], P('section', 'ep'), may hold values from -0.0625 to 0.0625
- w_up: bfloat16 [8, 32, 896, 1024], P('section', 'ep'), may hold values from -0.0625 to 0.0625
- w_down: bfloat16 [8, 32, 1024, 896], P('section', 'ep'), may hold values from -0.1875 to 0.1875
Outputs:
- grad_in: bfloat16 [8, 2, 2048, 7168], P('section', None, 'ep')
The draws below stay inside these ranges and needn't reach their ends.
Inputs may be any that keep to these rules, and one draw needn't show every extreme that they name: `routes`: each row names 2 different experts; within the 64 rows of one device for one direction no expert is named by more than 36 rows, and in some such blocks one expert is named by exactly 36. `slot_order`: within one device and direction each of 0 to 63 stands once.
All inputs are finite; a program needn't handle non-finite values.
Results may differ from the reference program's by a relative error of at most 0.011.
Values may be sent and summed in bfloat16 or wider, within the bound.
A program may use at most 128 MiB of HBM per device.

```python
import math
import jax
import jax.numpy as jnp
import numpy as np
from jax import lax

D = 7168
FF = 1024
EXPERTS = 4
TOPF = 2
TOK_DEV = 64
CAP = 36
GROUP = 8
TOKENS = 2048
N_SECTION = 8
N_EP = 32


def level_of(key, extent, pieces, smallest, largest):
    factor_of, own = 1.0, jax.random.fold_in(key, 6)
    for dim, blocks in pieces:
        heights = jnp.exp(jax.random.uniform(jax.random.fold_in(own, dim), (blocks,), jnp.float32, smallest / len(pieces), largest / len(pieces)))
        factor_of = factor_of * jnp.repeat(heights, extent[dim] // blocks).reshape([-1 if axis == dim else 1 for axis in range(len(extent))])
    return factor_of


def shared_out(own_key, own, number, rows, number_of, top, most, lean):
    ranking = jax.random.permutation(own_key, number_of)
    crowded, common = load_shares(number_of, rows * top, most, lean, True), load_shares(number_of, rows * top, most, lean, False)
    places = jnp.arange(number_of)

    def named(sizes, offset_by):
        used = int((sizes > 0).sum())
        fixed = max(1, used // 4)
        moved = fixed + (places - fixed + offset_by * (used - fixed)) % max(1, number_of - fixed)
        return jnp.zeros((number_of,), jnp.int32).at[ranking[jnp.where(places < fixed, places, moved)]].set(jnp.asarray(sizes, jnp.int32))

    sizes = jnp.where(number % 4 == 0, named(crowded, number // 4), named(common, number - number // 4 - 1))
    mixed = jax.random.permutation(jax.random.fold_in(own, 3), number_of)
    giver, sink = mixed[0:number_of // 2 * 2:2], mixed[1:number_of // 2 * 2:2]
    margin = jnp.minimum(sizes[giver] - 1, most - sizes[sink]) // 2
    margin = jnp.where((giver == ranking[0]) | (sink == ranking[0]) | (sizes[sink] == 0), 0, jnp.maximum(margin, 0))
    moved = jax.random.randint(jax.random.fold_in(own, 4), (number_of // 2,), 0, 1 << 20) % (margin + 1)
    sizes = sizes.at[giver].add(-moved).at[sink].add(moved)
    labels = jnp.searchsorted(jnp.cumsum(sizes), jnp.arange(rows * top), side="right").astype(jnp.int32)
    listing = labels.reshape(top, rows).T
    listing = listing[jax.random.permutation(jax.random.fold_in(own, 1), rows)]
    offset_by = jax.random.randint(jax.random.fold_in(own, 2), (rows, 1), 0, top)
    return jnp.take_along_axis(listing, (jnp.arange(top)[None, :] + offset_by) % top, axis=1)


def load_shares(amount, total, reach, lean, full):
    portions = [(1 << 20) // math.isqrt(rank ** lean) + 1 for rank in range(1, amount + 1)]
    largest = reach if full else min(reach, max(-(-total // amount), total * portions[0] // sum(portions)))
    least = 1 if total - largest >= amount - 1 else 0
    given, surplus = [largest] + [least] * (amount - 1), total - largest - least * (amount - 1)
    while surplus > 0:
        movable = [i for i in range(1, amount) if given[i] < largest] or [i for i in range(1, amount) if given[i] < reach]
        mass, remaining = sum([portions[i] for i in movable]), surplus
        for i in movable:
            more = min(reach - given[i], max(1, remaining * portions[i] // mass), surplus)
            given[i] = given[i] + more
            surplus = surplus - more
    return np.array(given)


def noise(stream_key, dims, deviation, most, pieces=(), kind=jnp.bfloat16):
    drawn = jax.random.normal(stream_key, dims, jnp.float32) * deviation
    if len(pieces) > 0:
        drawn = level_of(stream_key, dims, pieces, -0.22, 0.18) * drawn
    return jnp.clip(drawn, min=-most, max=most).astype(kind)


def setup_inputs(seed: int = 0) -> dict:
    key_list = jax.random.split(jax.random.key(seed), 10)
    handed = noise(key_list[0], (N_SECTION, 2, TOKENS, D), 1.0, 6.0, ((0, 8), (2, 32)))
    routes_keys = jax.random.split(jax.random.fold_in(key_list[1], 1), N_SECTION * 2 * TOKENS // TOK_DEV)
    routes_turns = jax.random.permutation(jax.random.fold_in(key_list[1], 3), N_SECTION * 2 * TOKENS // TOK_DEV)
    routes = jax.vmap(lambda own, number: shared_out(jax.random.fold_in(key_list[1], 2), own, number, TOK_DEV, EXPERTS, TOPF, CAP, 1))(routes_keys, routes_turns).reshape((N_SECTION, 2, TOKENS, TOPF))
    slot_order = jax.vmap(lambda own: jax.random.permutation(own, TOK_DEV))(jax.random.split(key_list[2], N_SECTION * 2 * N_EP)).reshape((N_SECTION, 2, N_EP, TOK_DEV)).astype(jnp.int32)
    gate_probs = jnp.clip(0.2 + 0.8 * jax.random.uniform(key_list[3], (N_SECTION, 2, TOKENS, TOPF), jnp.float32) ** level_of(key_list[3], (N_SECTION, 2, TOKENS, TOPF), ((0, 8), (2, 32)), -0.2, 0.2), 0.2, 1.0)
    saved_gate = noise(key_list[4], (N_SECTION, 2, N_EP, N_EP, CAP, FF // GROUP), 1.0, 6.0, ((0, 8), (2, 32)))
    saved_up = noise(key_list[5], (N_SECTION, 2, N_EP, N_EP, CAP, FF // GROUP), 1.0, 6.0, ((0, 8), (2, 32)))
    w_gate = noise(key_list[6], (N_SECTION, N_EP, D // GROUP, FF), D ** -0.5, 0.0625, ((0, 8), (1, 32)))
    w_up = noise(key_list[7], (N_SECTION, N_EP, D // GROUP, FF), D ** -0.5, 0.0625, ((0, 8), (1, 32)))
    w_down = noise(key_list[8], (N_SECTION, N_EP, FF, D // GROUP), FF ** -0.5, 0.1875, ((0, 8), (1, 32)))
    return {"handed": handed, "routes": routes, "slot_order": slot_order, "gate_probs": gate_probs, "saved_gate": saved_gate, "saved_up": saved_up, "w_gate": w_gate, "w_up": w_up, "w_down": w_down}


def slot_table(routing, sequence):
    expert_ids = jnp.arange(EXPERTS, dtype=jnp.int32)
    picked = (routing[:, :, None] == expert_ids[None, None, :]).astype(jnp.int32)
    named_count = jnp.sum(picked, axis=1)
    before = (sequence[None, :] < sequence[:, None]).astype(jnp.int32)
    counts = jnp.sum(before[:, :, None] * named_count[None, :, :], axis=1)
    return jnp.sum(counts[:, None, :] * picked, axis=2).astype(jnp.int32)


def reference(handed, routes, slot_order, gate_probs, saved_gate, saved_up, w_gate, w_up, w_down):
    group_size = N_EP // EXPERTS
    row_share = D // group_size
    unit_share = FF // group_size
    arriving = jnp.stack([jnp.roll(handed[:, 0], -1, axis=0), jnp.roll(handed[:, 1], 1, axis=0)], axis=1)
    sources = jnp.broadcast_to(jnp.arange(N_EP, dtype=jnp.int32)[:, None, None], (N_EP, TOK_DEV, TOPF))
    sections = []
    for section_index in range(N_SECTION):
        gate_full = w_gate[section_index].reshape(EXPERTS, D, FF).astype(jnp.float32)
        up_full = w_up[section_index].reshape(EXPERTS, D, FF).astype(jnp.float32)
        down_full = w_down[section_index].reshape(EXPERTS, group_size, FF, row_share)
        down_full = down_full.transpose(0, 2, 1, 3).reshape(EXPERTS, FF, D).astype(jnp.float32)
        directions = []
        for direction in range(2):
            grads = arriving[section_index, direction].reshape(N_EP, TOK_DEV, D)
            routing = routes[section_index, direction].reshape(N_EP, TOK_DEV, TOPF)
            slots = jax.vmap(slot_table)(routing, slot_order[section_index, direction])
            probs_here = gate_probs[section_index, direction].reshape(N_EP, TOK_DEV, TOPF)
            scaled = (probs_here[:, :, :, None] * grads[:, :, None, :].astype(jnp.float32)).astype(jnp.bfloat16)
            buffer = jnp.zeros((EXPERTS, N_EP, CAP, D), jnp.bfloat16).at[routing, sources, slots].set(scaled)
            row_block = buffer.reshape(EXPERTS, N_EP * CAP, D).astype(jnp.float32)
            hidden_grad = jnp.einsum("erd,efd->erf", row_block, down_full, precision=lax.Precision.HIGHEST)
            gate_vals = saved_gate[section_index, direction].reshape(EXPERTS, group_size, N_EP, CAP, unit_share)
            gate_vals = gate_vals.transpose(0, 2, 3, 1, 4).reshape(EXPERTS, N_EP * CAP, FF).astype(jnp.float32)
            up_vals = saved_up[section_index, direction].reshape(EXPERTS, group_size, N_EP, CAP, unit_share)
            up_vals = up_vals.transpose(0, 2, 3, 1, 4).reshape(EXPERTS, N_EP * CAP, FF).astype(jnp.float32)
            sigma = jax.nn.sigmoid(gate_vals)
            up_grad = (hidden_grad * gate_vals * sigma).astype(jnp.bfloat16)
            gate_grad = (hidden_grad * up_vals * sigma * (1.0 + gate_vals * (1.0 - sigma))).astype(jnp.bfloat16)
            combined = jnp.einsum("erf,edf->erd", gate_grad.astype(jnp.float32), gate_full, precision=lax.Precision.HIGHEST)
            combined = combined + jnp.einsum("erf,edf->erd", up_grad.astype(jnp.float32), up_full, precision=lax.Precision.HIGHEST)
            combined = combined.astype(jnp.bfloat16).reshape(EXPERTS, N_EP, CAP, D)
            picked_rows = combined[routing, sources, slots]
            summed = jnp.sum(picked_rows.astype(jnp.float32), axis=2).astype(jnp.bfloat16)
            directions.append(summed.reshape(N_EP * TOK_DEV, D))
        sections.append(jnp.stack(directions))
    return jnp.stack(sections)
```

```python
import functools

import jax
import jax.numpy as jnp
from jax import lax
from jax.experimental import pallas as pl
from jax.experimental.pallas import tpu as pltpu
from jax.sharding import PartitionSpec as P

MESH = pl.DeviceIdType.MESH
BF = jnp.bfloat16
F32 = jnp.float32
CAP = 36
TOK = 64
SL = 896
FF = 1024
CH = 4 * CAP
NCH = 16
NT = (((1,), (1,)), ((), ()))

ORDER = (
    ("disp", 0),
    ("core", 6),
    ("xhop", 5),
    ("exp", 3),
    ("act", 4),
    ("sum", 3),
    ("out", 6),
)


def kernel(
    meta, handed, gate, up, w1, w3, w2, out,
    A, DS, R, PB, RS1, SZS, SZR, OWN, H, ES, B, OS, MR, T, TT, OH, RP, OHT, W1P, W3P, W2P, GV, UV,
    w_sem, gu_sem, m_s, m_r, a_s, a_r, ds_s, r_r, rs_s, rs_r, sz_s, sz_r, hz_s, hz_r,
    hx_s, hx_r, hc_s, hc_r, es_s, b_r, o_s, o_r, ol_s,
):
    s = lax.axis_index("section")
    ep = lax.axis_index("ep")
    z = ep // 4
    xl = (ep // 2) % 2
    c = ep % 2
    pid = ep % 4
    e = z // 2
    zp = z % 2
    pos2 = c * 2 + xl
    pos = pos2 * 2 + zp
    after = (s + 1) % 8
    before = (s + 7) % 8
    zpart = (z + 1 - 2 * zp) * 4 + pid
    xpart = z * 4 + (1 - xl) * 2 + c
    cpart = z * 4 + xl * 2 + 1 - c

    def rcopy(src, dst, ssem, rsem, epi, sec=None):
        return pltpu.make_async_remote_copy(
            src_ref=src, dst_ref=dst, send_sem=ssem, recv_sem=rsem,
            device_id={"section": s if sec is None else sec, "ep": epi}, device_id_type=MESH,
        )

    def lanes(start, size):
        return pl.ds(pl.multiple_of(start, 128), size)

    loads = []
    for p in range(8):
        j = (p & 1) * 4 + ((p >> 1) & 1) * 2 + (p >> 2)
        here, there = pl.ds(p * 128, 128), pl.ds(j * 128, 128)
        loads.append(pltpu.make_async_copy(w2.at[there, :], W2P.at[here, :], w_sem.at[p]))
        loads.append(pltpu.make_async_copy(w1.at[:, there], W1P.at[:, here], w_sem.at[8 + p]))
        loads.append(pltpu.make_async_copy(w3.at[:, there], W3P.at[:, here], w_sem.at[16 + p]))
    loads.append(pltpu.make_async_copy(gate, GV, gu_sem.at[0]))
    loads.append(pltpu.make_async_copy(up, UV, gu_sem.at[1]))

    bar = pltpu.get_barrier_semaphore()

    def greet(sec, epi):
        pl.semaphore_signal(bar, inc=1, device_id={"section": sec, "ep": epi}, device_id_type=MESH)

    for k in range(4):
        greet(after, z * 4 + k)
        greet(before, z * 4 + k)
    for k in range(1, 4):
        greet(s, z * 4 + (pid + k) % 4)
    for k in range(1, 8):
        greet(s, ((z + k) % 8) * 4 + pid)
    pl.semaphore_wait(bar, 18)

    def meta_copy(k):
        other = (pid + k) % 4
        return rcopy(meta, MR.at[pl.ds(pid * 16, 16), :], m_s.at[k], m_r.at[pid], z * 4 + other)

    for k in range(1, 4):
        meta_copy(k).start()

    def relay(d, turn, k):
        q = zp if turn == 0 else 1 - zp
        other = (pid + k) % 4
        return rcopy(
            handed.at[d, :, lanes((q * 4 + other) * SL, SL)],
            A.at[d, q, pl.ds(pl.multiple_of(pid * TOK, TOK), TOK), :],
            a_s.at[(d * 2 + turn) * 4 + k],
            a_r.at[(d * 2 + turn) * 4 + pid],
            z * 4 + other,
            before if d == 0 else after,
        )

    for d in range(2):
        for turn in range(2):
            for k in range(4):
                relay(d, turn, k).start()
    for load in loads:
        load.start()

    MR[pl.ds(pl.multiple_of(pid * 16, 16), 16), :] = meta[...]
    for k in range(1, 4):
        other = (pid + k) % 4
        rcopy(meta, MR.at[pl.ds(other * 16, 16), :], m_s.at[k], m_r.at[other], zpart).wait_recv()
    rows = MR[...]
    cols = jnp.concatenate([rows, rows], axis=0).T
    lane = lax.broadcasted_iota(jnp.int32, (TOK, 128), 1)
    for src in range(4):
        acc = jnp.zeros((TOK, 128), F32)
        for d in range(2):
            base = src * 16 + d * 8
            r_e0, r_e1, r_ord = (rows[base + f : base + f + 1, :] for f in range(3))
            c_ord = cols[:TOK, base + 2 : base + 3]
            for k in range(2):
                c_e = cols[:TOK, base + k : base + k + 1]
                earlier = (r_ord < c_ord) & ((r_e0 == c_e) | (r_e1 == c_e)) & (lane < TOK)
                count = jnp.sum(jnp.where(earlier, 1.0, 0.0), axis=1, keepdims=True)
                target = c_e * float(CH) + float(src * CAP) + count
                acc = jnp.where(lane == d * 2 + k, target, acc)
                prob = cols[:TOK, base + 3 + k : base + 4 + k]
                acc = jnp.where(lane == 4 + d * 2 + k, prob, acc)
        T[src * TOK : (src + 1) * TOK, :] = acc
    TT[...] = T[...].T
    for d in range(2):
        row0, row1 = TT[d * 2 : d * 2 + 1, :], TT[d * 2 + 1 : d * 2 + 2, :]
        p0, p1 = TT[4 + d * 2 : 5 + d * 2, :], TT[5 + d * 2 : 6 + d * 2, :]
        for ex in range(4):
            ids = (lax.broadcasted_iota(jnp.int32, (CH, 256), 0) + ex * CH).astype(F32)
            hit0, hit1 = ids == row0, ids == row1
            OH[d * 4 + ex] = jnp.where(hit0 | hit1, 1.0, 0.0).astype(BF)
            scale = jnp.sum(
                jnp.where(hit0, p0, 0.0) + jnp.where(hit1, p1, 0.0), axis=1, keepdims=True
            )
            RP[d * 4 + ex] = jnp.broadcast_to(scale, (CH, 128))
        ids = lax.broadcasted_iota(jnp.int32, (256, 4 * CH), 1).astype(F32)
        hit = (ids == T[:, d * 2 : d * 2 + 1]) | (ids == T[:, d * 2 + 1 : d * 2 + 2])
        OHT[d] = jnp.where(hit, 1.0, 0.0).astype(BF)

    def offset(i):
        half = (i + 1) // 2
        return jnp.where(i % 2 == 1, half, 8 - half)

    def source(n):
        d = n // 8
        return d, (2 * e + offset(n % 8)) % 8

    def wait_relay(d, turn):
        q = zp if turn == 0 else 1 - zp
        for k in range(4):
            rcopy(
                A.at[d, q, pl.ds(k * TOK, TOK), :], A.at[d, q, pl.ds(k * TOK, TOK), :],
                a_s.at[0], a_r.at[(d * 2 + turn) * 4 + k], zpart,
            ).wait_recv()

    def disp(n):
        for d_ in range(2):
            for turn in range(2):
                @pl.when(n == d_ * 8 + turn)
                def _():
                    wait_relay(d_, turn)

        d, m = n // 8, n % 8
        zd = (z + offset(m)) % 8
        ed, qd = zd // 2, zd % 2
        picked = jnp.dot(OH[d * 4 + ed], A[d, qd], preferred_element_type=F32)
        scaled = (picked * RP[d * 4 + ed][:, 0:1]).astype(BF)

        @pl.when(m == 0)
        def _():
            R[d * 8 + z] = scaled

        @pl.when(m != 0)
        def _():
            DS[d * 8 + zd] = scaled
            rcopy(
                DS.at[d * 8 + zd], R.at[d * 8 + z], ds_s.at[d * 8 + zd], r_r.at[d * 8 + z],
                zd * 4 + pid,
            ).start()

    def partial(q, k):
        other = (pid + k) % 4
        wide = lanes(((other % 2) * 2 + other // 2) * 256, 256)
        return rcopy(
            PB.at[q, :, wide], RS1.at[q, pid], rs_s.at[q * 4 + k], rs_r.at[q * 4 + pid],
            z * 4 + other,
        )

    def exp(n):
        d, zs = source(n)
        q = d * 8 + zs

        @pl.when(zs != z)
        def _():
            rcopy(R.at[q], R.at[q], ds_s.at[q], r_r.at[q], zpart).wait_recv()

        PB[q] = lax.dot_general(R[q], W2P[...], NT, preferred_element_type=F32).astype(BF)
        for k in range(1, 4):
            partial(q, k).start()

    def zsum(q):
        return rcopy(SZS.at[q], SZR.at[q], sz_s.at[q], sz_r.at[q], zpart)

    def sum_(n):
        d, zs = source(n)
        q = d * 8 + zs
        total = PB[q, :, lanes(pos2 * 256, 256)].astype(F32)
        for k in range(1, 4):
            other = (pid + k) % 4
            rcopy(
                RS1.at[q, other], RS1.at[q, other], rs_s.at[q * 4], rs_r.at[q * 4 + other], zpart
            ).wait_recv()
            total = total + RS1[q, other].astype(F32)
        low, high = total[:, :128], total[:, 128:]
        SZS[q] = jnp.where(zp == 0, high, low).astype(BF)
        OWN[q] = jnp.where(zp == 0, low, high)
        zsum(q).start()

    def grads(q, width, start, ssem, rsem, to):
        part = H.at[q, :, :, lanes(start, width)]
        return rcopy(part, part, ssem.at[q], rsem.at[q], to)

    def act(n):
        d, zs = source(n)
        q = d * 8 + zs
        zsum(q).wait_recv()
        grad = OWN[q] + SZR[q].astype(F32)
        g, u = GV[q].astype(F32), UV[q].astype(F32)
        sigma = jax.nn.sigmoid(g)
        here = lanes(pos * 128, 128)
        H[q, 0, :, here] = (grad * u * sigma * (1.0 + g * (1.0 - sigma))).astype(BF)
        H[q, 1, :, here] = (grad * g * sigma).astype(BF)
        grads(q, 128, pos * 128, hz_s, hz_r, zpart).start()

    def xhop(n):
        d, zs = source(n)
        q = d * 8 + zs
        grads(q, 128, (pos2 * 2 + 1 - zp) * 128, hz_s, hz_r, zpart).wait_recv()
        grads(q, 256, pos2 * 256, hx_s, hx_r, xpart).start()

    def core(n):
        d, zs = source(n)
        q = d * 8 + zs
        grads(q, 256, (c * 2 + 1 - xl) * 256, hx_s, hx_r, xpart).wait_recv()
        grads(q, 512, c * 512, hc_s, hc_r, cpart).start()

    def back(q, d, zs):
        return rcopy(ES.at[q], B.at[d, zp, e], es_s.at[q], b_r.at[d * 8 + z], zs * 4 + pid)

    def out_(n):
        d, zs = source(n)
        q = d * 8 + zs
        grads(q, 512, (1 - c) * 512, hc_s, hc_r, cpart).wait_recv()
        result = lax.dot_general(H[q, 0], W1P[...], NT, preferred_element_type=F32)
        result = result + lax.dot_general(H[q, 1], W3P[...], NT, preferred_element_type=F32)

        @pl.when(zs == z)
        def _():
            B[d, zp, e] = result.astype(BF)

        @pl.when(zs != z)
        def _():
            ES[q] = result.astype(BF)
            back(q, d, zs).start()

    def final(d, par, k):
        other = (pid + k) % 4
        return rcopy(
            OS.at[d, par, pl.ds(pl.multiple_of(other * TOK, TOK), TOK), :],
            out.at[d, :, lanes((par * 4 + pid) * SL, SL)],
            o_s.at[(d * 2 + par) * 4 + k], o_r.at[(d * 2 + par) * 4 + pid], z * 4 + other,
        )

    def final_own(d, par):
        return pltpu.make_async_copy(
            OS.at[d, par, pl.ds(pl.multiple_of(pid * TOK, TOK), TOK), :],
            out.at[d, :, lanes((par * 4 + pid) * SL, SL)],
            ol_s.at[d * 2 + par],
        )

    def combine(d):
        for par in range(2):
            for ex in range(4):
                zo = ex * 2 + par

                @pl.when(zo != z)
                def _():
                    rcopy(
                        B.at[d, par, ex], B.at[d, par, ex], es_s.at[0], b_r.at[d * 8 + zo], zpart
                    ).wait_recv()

            table = B[d, par].reshape(4 * CH, SL)
            OS[d, par] = jnp.dot(OHT[d], table, preferred_element_type=F32).astype(BF)
            for k in range(1, 4):
                final(d, par, k).start()
            final_own(d, par).start()

    for load in loads:
        load.wait()

    stages = {
        "disp": disp, "exp": exp, "sum": sum_, "act": act, "xhop": xhop, "core": core, "out": out_,
    }
    longest = max(lag for _, lag in ORDER)

    def step(t, carry):
        for name, lag in ORDER:
            n = t - lag

            @pl.when((n >= 0) & (n < NCH))
            def _():
                stages[name](jnp.clip(n, 0, NCH - 1))

        @pl.when(t == 8 + longest + 1)
        def _():
            combine(0)

        return carry

    lax.fori_loop(0, NCH + longest, step, 0)
    combine(1)

    for d in range(2):
        for par in range(2):
            final_own(d, par).wait()
            for k in range(1, 4):
                other = (pid + k) % 4
                rcopy(
                    out.at[d, :, lanes((par * 4 + other) * SL, SL)],
                    out.at[d, :, lanes((par * 4 + other) * SL, SL)],
                    o_s.at[0], o_r.at[(d * 2 + par) * 4 + other], zpart,
                ).wait_recv()
                final(d, par, k).wait_send()
            for k in range(4):
                relay(d, par, k).wait_send()
    for k in range(1, 4):
        meta_copy(k).wait_send()

    def drain(n, carry):
        d, zs = source(n)
        q = d * 8 + zs
        for k in range(1, 4):
            partial(q, k).wait_send()
        zsum(q).wait_send()
        grads(q, 128, pos * 128, hz_s, hz_r, zpart).wait_send()
        grads(q, 256, pos2 * 256, hx_s, hx_r, xpart).wait_send()
        grads(q, 512, c * 512, hc_s, hc_r, cpart).wait_send()

        @pl.when(zs != z)
        def _():
            rcopy(DS.at[q], R.at[d * 8 + z], ds_s.at[q], r_r.at[d * 8 + z], zpart).wait_send()
            back(q, d, zs).wait_send()

        return carry

    lax.fori_loop(0, NCH, drain, 0)


def local(handed, routes, slot_order, gate_probs, saved_gate, saved_up, w_gate, w_up, w_down):
    fields = jnp.concatenate(
        [
            routes[0].transpose(0, 2, 1).astype(F32),
            slot_order[0].astype(F32),
            gate_probs[0].transpose(0, 2, 1),
        ],
        axis=1,
    )
    meta = jnp.pad(fields, ((0, 0), (0, 3), (0, 128 - TOK))).reshape(16, 128)
    gate = saved_gate.reshape(NCH, CH, 128)
    up = saved_up.reshape(NCH, CH, 128)
    anyspace = pl.BlockSpec(memory_space=pl.ANY)
    dma = pltpu.SemaphoreType.DMA
    result = pl.pallas_call(
        kernel,
        out_shape=jax.ShapeDtypeStruct((2, TOK, 8 * SL), BF),
        in_specs=[pl.BlockSpec(memory_space=pltpu.VMEM)] + [anyspace] * 6,
        out_specs=anyspace,
        scratch_shapes=[
            pltpu.VMEM((2, 2, 256, SL), BF),
            pltpu.VMEM((NCH, CH, SL), BF),
            pltpu.VMEM((NCH, CH, SL), BF),
            pltpu.VMEM((NCH, CH, FF), BF),
            pltpu.VMEM((NCH, 4, CH, 256), BF),
            pltpu.VMEM((NCH, CH, 128), BF),
            pltpu.VMEM((NCH, CH, 128), BF),
            pltpu.VMEM((NCH, CH, 128), F32),
            pltpu.VMEM((NCH, 2, CH, FF), BF),
            pltpu.VMEM((NCH, CH, SL), BF),
            pltpu.VMEM((2, 2, 4, CH, SL), BF),
            pltpu.VMEM((2, 2, 256, SL), BF),
            pltpu.VMEM((64, 128), F32),
            pltpu.VMEM((256, 128), F32),
            pltpu.VMEM((128, 256), F32),
            pltpu.VMEM((8, CH, 256), BF),
            pltpu.VMEM((8, CH, 128), F32),
            pltpu.VMEM((2, 256, 4 * CH), BF),
            pltpu.VMEM((SL, FF), BF),
            pltpu.VMEM((SL, FF), BF),
            pltpu.VMEM((FF, SL), BF),
            pltpu.VMEM((NCH, CH, 128), BF),
            pltpu.VMEM((NCH, CH, 128), BF),
            dma((24,)), dma((2,)),
            dma((4,)), dma((4,)),
            dma((16,)), dma((16,)),
            dma((NCH,)), dma((NCH,)),
            dma((4 * NCH,)), dma((4 * NCH,)),
            dma((NCH,)), dma((NCH,)),
            dma((NCH,)), dma((NCH,)),
            dma((NCH,)), dma((NCH,)),
            dma((NCH,)), dma((NCH,)),
            dma((NCH,)), dma((NCH,)),
            dma((16,)), dma((16,)),
            dma((4,)),
        ],
        compiler_params=pltpu.CompilerParams(
            collective_id=0, has_side_effects=True, vmem_limit_bytes=62 * 1024 * 1024
        ),
    )(meta, handed[0], gate, up, w_gate[0, 0], w_up[0, 0], w_down[0, 0])
    return result[None]


def solution(mesh):
    in_specs = (
        P("section", None, "ep", None),
        P("section", None, "ep", None),
        P("section", None, "ep", None),
        P("section", None, "ep", None),
        P("section", None, "ep", None, None, None),
        P("section", None, "ep", None, None, None),
        P("section", "ep", None, None),
        P("section", "ep", None, None),
        P("section", "ep", None, None),
    )
    out_specs = P("section", None, "ep", None)
    return jax.shard_map(local, mesh=mesh, in_specs=in_specs, out_specs=out_specs, check_vma=False)
```
